32 devices in a mesh: gx: 2 (over y), gy: 4 (over z), gz: 4 (over x, core).
Axes of the slice: x: 2, y: 2, z: 4, core: 2. Of those that a mesh axis runs over, the one named last changes fastest.
Arguments:
- gas_temp: float32 [128, 128, 1024], P('gz', 'gx', 'gy'), may hold values from 1 to 8
- fuel_frac: float32 [128, 128, 1024], P('gz', 'gx', 'gy'), may hold values from 0 to 1
- velocity: float32 [3, 128, 128, 1024], P(None, 'gz', 'gx', 'gy'), may hold values from -3 to 3
- wall_flags: int32 [128, 1024], P('gx', 'gy'), may hold values 0 or 1
- solid_temp: float32 [64, 256, 2048], P(None, ('gx', 'gy'), 'gz'), may hold values from 1 to 3
- diffusivity: float32 [64, 256, 2048], P(None, ('gx', 'gy'), 'gz'), may hold values from 0.03 to 0.15
- gas_owner: int32 [256, 2048], P(('gx', 'gy'), 'gz'), may hold values from 0 to 131071, as said below
Outputs:
- gas_temp_new: float32 [128, 128, 1024], P('gz', 'gx', 'gy')
- fuel_frac_new: float32 [128, 128, 1024], P('gz', 'gx', 'gy')
- solid_temp_new: float32 [64, 256, 2048], P(None, ('gx', 'gy'), 'gz')
The draws below stay inside these ranges and needn't reach their ends.
Inputs may be any that keep to these rules, and one draw needn't show every extreme that they name: gas_owner[p, q] = a * 1024 + b where a differs from p // 2 by at most 4 modulo 128 and b differs from q // 2 by at most 4 modulo 1024; both offsets reach 4 in both directions.
All inputs are finite; a program needn't handle non-finite values. No bound on the sum of `wall_flags` on one device may be relied on, other than what follows from the above.
Results may differ from the reference program's by a relative error of at most 0.00002.
Values sent between devices are 32-bit elements; how exact they have to be, the bound alone decides.
A program may use at most 128 MiB of HBM per device.

```python
import math
import jax
import jax.numpy as jnp

SZ = 64
SUBSTEPS = 4
DISP = 4
NX = 128
NY = 1024
NZ = 128
SX = 256
SY = 2048


def draw_gas_owner(key, part):
    key_rows = jax.random.fold_in(key, 11)
    key_cols = jax.random.fold_in(key, 23)
    shift_rows = jax.random.randint(key_rows, (SX, SY), -DISP, DISP + 1)
    shift_cols = jax.random.randint(key_cols, (SX, SY), -DISP, DISP + 1)
    base_rows = jnp.arange(SX, dtype=jnp.int32)[:, None] // 2
    base_cols = jnp.arange(SY, dtype=jnp.int32)[None, :] // 2
    gas_row = (base_rows + shift_rows) % NX
    gas_col = (base_cols + shift_cols) % NY
    return (gas_row * NY + gas_col).astype(jnp.int32)


def touch_ends(entries, own_key, least, high):
    extent = entries.shape
    spot = [jax.random.randint(jax.random.fold_in(own_key, axis), (), 0, extent[axis]) for axis in range(len(extent))]
    entries = entries.at[tuple(spot)].set(least)
    longest = extent.index(max(extent))
    spot[longest] = (spot[longest] + 1) % extent[longest]
    return entries.at[tuple(spot)].set(high)


def shard_levels(key, extent, pieces, low, largest):
    def one(dim, parts):
        draws = jax.random.uniform(jax.random.fold_in(jax.random.fold_in(key, 6), dim), (parts,), jnp.float32, low / len(pieces), largest / len(pieces))
        return jnp.repeat(jnp.exp(draws), extent[dim] // parts).reshape((-1,) + (1,) * (len(extent) - dim - 1))

    factor_of = one(*pieces[0])
    for cut in pieces[1:]:
        factor_of = factor_of * one(*cut)
    return factor_of


def centred(own_key, shape, spread, bound, split=(), kind=jnp.bfloat16):
    array = jax.random.normal(own_key, shape, jnp.float32) * spread
    if len(split) > 0:
        array = shard_levels(own_key, shape, split, -0.22, 0.18) * array
    return jnp.clip(array, min=-bound, max=bound).astype(kind)


def setup_inputs(seed: int = 0) -> dict:
    keys = jax.random.split(jax.random.key(seed), 8)
    return {
        "gas_temp": jnp.clip(1.0 + 7.0 * jax.random.uniform(keys[0], (NZ, NX, NY), jnp.float32) ** shard_levels(keys[0], (NZ, NX, NY), ((0, 4), (1, 2), (2, 4)), -0.2, 0.2), 1.0, 8.0),
        "fuel_frac": jnp.clip(1.0 * jax.random.uniform(keys[1], (NZ, NX, NY), jnp.float32) ** shard_levels(keys[1], (NZ, NX, NY), ((0, 4), (1, 2), (2, 4)), -0.2, 0.2), 0.0, 1.0),
        "velocity": centred(keys[2], (3, NZ, NX, NY), 0.5, 3.0, ((1, 4), (2, 2), (3, 4)), jnp.float32),
        "wall_flags": touch_ends((jax.random.randint(keys[3], (NX, NY), 0, 4) < 3).astype(jnp.int32), jax.random.fold_in(keys[3], 1), 0, 1),
        "solid_temp": jnp.clip(1.0 + 2.0 * jax.random.uniform(keys[4], (SZ, SX, SY), jnp.float32) ** shard_levels(keys[4], (SZ, SX, SY), ((1, 8), (2, 4)), -0.2, 0.2), 1.0, 3.0),
        "diffusivity": jnp.clip(jnp.exp(math.log(0.15) - 1.609438 * jax.random.uniform(keys[5], (SZ, SX, SY), jnp.float32) ** shard_levels(keys[5], (SZ, SX, SY), ((1, 8), (2, 4)), -0.2, 0.2)), 0.03, 0.15),
        "gas_owner": draw_gas_owner(jax.random.fold_in(keys[7], 71), 0),
    }


FILM_COEF = 0.15
SOURCE_GAIN = 0.25
COOLANT = 1.0
DIFFUSE_TEMP = 0.2
DIFFUSE_FUEL = 0.15
TIME_STEP = 0.2
RATE_CONST = 1.0
ACTIVATION = 4.0
HEAT_RELEASE = 3.0


def gas_update(fields, z_below, z_above, x_below, x_above, y_below, y_above, velocity):
    advect = 0.5 * (velocity[0] * (z_above - z_below) + velocity[1] * (x_above - x_below) + velocity[2] * (y_above - y_below))
    nearby = z_below + z_above + x_below + x_above + y_below + y_above
    reaction = RATE_CONST * fields[1] * jnp.exp(-ACTIVATION / fields[0])
    temp_new = fields[0] + TIME_STEP * (-advect[0] + DIFFUSE_TEMP * (nearby[0] - 6.0 * fields[0]) + HEAT_RELEASE * reaction)
    fuel_new = fields[1] + TIME_STEP * (-advect[1] + DIFFUSE_FUEL * (nearby[1] - 6.0 * fields[1]) - reaction)
    return temp_new, fuel_new


def solid_step(solid_now, diffusivity, wall_flux):
    bottom_ghost = jnp.full_like(solid_now[:1], COOLANT)
    z_below = jnp.concatenate([solid_now[:1], solid_now[:-1]], 0)
    z_above = jnp.concatenate([solid_now[1:], bottom_ghost], 0)
    nearby = z_below + z_above + jnp.roll(solid_now, 1, 1) + jnp.roll(solid_now, -1, 1)
    nearby = nearby + jnp.roll(solid_now, 1, 2) + jnp.roll(solid_now, -1, 2)
    solid_next = solid_now + diffusivity * (nearby - 6.0 * solid_now)
    return solid_next.at[0].add(SOURCE_GAIN * wall_flux)


def reference(gas_temp, fuel_frac, velocity, wall_flags, solid_temp, diffusivity, gas_owner):
    gas_face = gas_temp[0]
    film = FILM_COEF * wall_flags.astype(jnp.float32) * gas_face ** 0.7
    gas_at = gas_face.reshape(-1)[gas_owner]
    film_at = film.reshape(-1)[gas_owner]
    wall_flux = film_at * (gas_at - solid_temp[0])
    solid_now = solid_temp
    for substep in range(SUBSTEPS):
        solid_now = solid_step(solid_now, diffusivity, wall_flux)
    surface = solid_now[0]
    wall_temp = 0.25 * surface.reshape(NX, 2, NY, 2).sum(axis=(1, 3))
    fields = jnp.stack([gas_temp, fuel_frac])
    low_temp = jnp.where(wall_flags == 1, 2.0 * wall_temp - gas_temp[0], gas_temp[0])
    low_layer = jnp.stack([low_temp, fuel_frac[0]])
    z_below = jnp.concatenate([low_layer[:, None], fields[:, :-1]], 1)
    z_above = jnp.concatenate([fields[:, 1:], fields[:, -1:]], 1)
    temp_new, fuel_new = gas_update(fields, z_below, z_above,
                                    jnp.roll(fields, 1, 2), jnp.roll(fields, -1, 2),
                                    jnp.roll(fields, 1, 3), jnp.roll(fields, -1, 3), velocity)
    return temp_new, fuel_new, solid_now
```

```python
import functools

import jax
import jax.numpy as jnp
from jax import lax
from jax.experimental import pallas as pl
from jax.experimental.pallas import tpu as pltpu
from jax.sharding import PartitionSpec as P

SUBSTEPS = 4
DISP = 4

FILM_COEF = 0.15
SOURCE_GAIN = 0.25
COOLANT = 1.0
DIFFUSE_TEMP = 0.2
DIFFUSE_FUEL = 0.15
TIME_STEP = 0.2
RATE_CONST = 1.0
ACTIVATION = 4.0
HEAT_RELEASE = 3.0

LANES = 128
SUB = 8
CHUNK = 8
GROUP = LANES // CHUNK
HALO = SUBSTEPS
SPAN = 2 * DISP + 1
MESH = pl.DeviceIdType.MESH
ANY = pl.BlockSpec(memory_space=pl.ANY)


def iota(shape, dim):
    return lax.broadcasted_iota(jnp.int32, shape, dim)


def lanes_of(x, idx):
    return jnp.take_along_axis(x, idx, axis=1, mode="promise_in_bounds")


def mega_kernel(
    mesh_shape,
    temp_in,
    fuel_in,
    vel_in,
    flags_in,
    solid_in,
    diff_in,
    owner_in,
    temp_out,
    fuel_out,
    solid_out,
    G,
    V,
    FL,
    A,
    B,
    D,
    TO,
    FO,
    OW,
    E,
    EN,
    CO,
    CN,
    MS,
    MR,
    ZS,
    ZR,
    XS,
    XR,
    YS,
    YR,
    GS,
    GB,
    DW,
    F,
    WS,
    WR,
    load_s,
    load_d,
    load_g,
    load_m,
    out_sem,
    row_send,
    row_recv,
    zone_send,
    zone_recv,
    edge_send,
    edge_recv,
    code_send,
    code_recv,
    y_send,
    y_recv,
    x_send,
    x_recv,
    z_send,
    z_recv,
    face_send,
    face_recv,
    wt_send,
    wt_recv,
):
    nx, ny, nz = mesh_shape
    gx, gy, gz = lax.axis_index("gx"), lax.axis_index("gy"), lax.axis_index("gz")
    layers_g, rows_g, cols_g = temp_in.shape
    layers, rows, cols = solid_in.shape
    chunks = layers // CHUNK
    wt = cols // LANES
    gt = cols_g // LANES
    units = wt * CHUNK
    strip = rows // 2
    top = SUB
    rtiles = rows // SUB
    gtiles = rows_g // SUB
    steps = SUBSTEPS * chunks
    lane = iota((SUB, LANES), 1)

    def dev(x, y, z):
        return (x, y, z)

    def ring(i, n, by):
        return lax.rem(i + n + by, n)

    line = gx * ny + gy
    line_next, line_prev = ring(line, nx * ny, 1), ring(line, nx * ny, -1)
    row_dev = (
        dev(lax.div(line_next, ny), lax.rem(line_next, ny), gz),
        dev(lax.div(line_prev, ny), lax.rem(line_prev, ny), gz),
    )
    col_dev = (dev(gx, gy, ring(gz, nz, 1)), dev(gx, gy, ring(gz, nz, -1)))
    y_dev = (dev(gx, ring(gy, ny, 1), gz), dev(gx, ring(gy, ny, -1), gz))
    x_dev = (dev(ring(gx, nx, 1), gy, gz), dev(ring(gx, nx, -1), gy, gz))

    def remote(src, dst, ssem, rsem, to):
        return pltpu.make_async_remote_copy(
            src_ref=src, dst_ref=dst, send_sem=ssem, recv_sem=rsem, device_id=to, device_id_type=MESH
        )

    def load_gas(f, src, k):
        return pltpu.make_async_copy(
            src.at[:, :, pl.ds(k * LANES, LANES)],
            G.at[f, pl.ds(1, layers_g), k, pl.ds(top, rows_g), :],
            load_g.at[f, k],
        )

    def load_wall(src, c, k):
        if src is solid_in:
            dst = A.at[c, pl.ds(k * CHUNK, CHUNK), pl.ds(top, rows), :]
            sem = load_s.at[c, k]
        else:
            dst = D.at[c, pl.ds(k * CHUNK, CHUNK), :, :]
            sem = load_d.at[c, k]
        return pltpu.make_async_copy(src.at[pl.ds(c * CHUNK, CHUNK), :, pl.ds(k * LANES, LANES)], dst, sem)

    load_flags = pltpu.make_async_copy(flags_in, FL, load_m.at[0])
    load_owner = pltpu.make_async_copy(owner_in, OW, load_m.at[1])
    load_vel = pltpu.make_async_copy(vel_in, V, load_m.at[2])

    def store_wall(c, k):
        return pltpu.make_async_copy(
            A.at[c, pl.ds(k * CHUNK, CHUNK), pl.ds(top, rows), :],
            solid_out.at[pl.ds(c * CHUNK, CHUNK), :, pl.ds(k * LANES, LANES)],
            out_sem.at[2, c, k],
        )

    def store_gas(f, z):
        src, dst = ((TO, temp_out), (FO, fuel_out))[f]
        return pltpu.make_async_copy(src.at[z], dst.at[z], out_sem.at[f, lax.div(z, wt), lax.rem(z, wt)])

    def row_copy(t, c, way):
        count = pl.ds(0, units + 1)
        return remote(
            MS.at[way, t, c, count, :],
            MR.at[way, t, c, count, :],
            row_send.at[way, t, c],
            row_recv.at[way, t, c],
            row_dev[way],
        )

    def first_copy(c, way):
        count = pl.ds(0, units)
        return remote(
            MS.at[way, 0, c, count, :],
            MR.at[way, 0, c, count, :],
            row_send.at[way, 0, c],
            row_recv.at[way, 0, c],
            row_dev[way],
        )

    def zone_copy(way):
        return remote(ZS.at[way], ZR.at[way], zone_send.at[way], zone_recv.at[way], row_dev[way])

    inner = ((top + rows - 1), top)
    outer = ((top - 1), top + rows)

    def pack_rows(src, t, c, count):
        for way in range(2):
            for u in range(count):
                MS[way, t, c, u : u + 1, :] = src[c, u, inner[way] : inner[way] + 1, :]

    def unpack_rows(dst, t, c, count):
        for way in range(2):
            for u in range(count):
                dst[c, u, outer[way] : outer[way] + 1, :] = MR[way, t, c, u : u + 1, :]

    def edge_copy(c, way):
        return remote(E.at[c], EN.at[way, c], edge_send.at[way, c], edge_recv.at[way, c], col_dev[way])

    def code_copy(way):
        return remote(CO, CN.at[way], code_send.at[way], code_recv.at[way], col_dev[way])

    def y_copy(way):
        return remote(YS.at[way], YR.at[way], y_send.at[way], y_recv.at[way], y_dev[way])

    def x_copy(way):
        return remote(XS.at[way], XR.at[way], x_send.at[way], x_recv.at[way], x_dev[way])

    inner_g = (top + rows_g - 1, top)
    outer_g = (top - 1, top + rows_g)

    def z_copy(f, way):
        src, dst = ((layers_g, 0), (1, layers_g + 1))[way]
        return remote(
            G.at[f, src, :, pl.ds(top, rows_g), :],
            G.at[f, dst, :, pl.ds(top, rows_g), :],
            z_send.at[f, way],
            z_recv.at[f, way],
            col_dev[way],
        )

    has_z = (gz < nz - 1, gz > 0)

    segs = (
        (0, 0, gt, 1),
        (1, gt - 1, 1, 0),
        (-1, 0, 1, gt + 1),
    )
    parts = []
    for j in range(ny):
        r0, r1 = max(0, strip * j - SUB), min(rows_g, strip * (j + 1) + SUB)
        parts.append((0, j, r0, r1 - r0, r0 - (strip * j - SUB)))
    parts.append((1, 0, rows_g - SUB, SUB, 0))
    parts.append((-1, ny - 1, 0, SUB, strip + SUB))

    def face_pieces():
        for n, (dx, j, r0, count, d0) in enumerate(parts):
            for m, (dk, s0, tiles, t0) in enumerate(segs):
                k = ring(gy, ny, dk)
                src = GS.at[pl.ds(s0, tiles), pl.ds(r0, count), :]
                dst = GB.at[pl.ds(t0, tiles), pl.ds(d0, count), :]
                copy = remote(src, dst, face_send.at[n, m], face_recv.at[m], dev(ring(gx, nx, dx), j, k))
                me = (k == 0) & (gy == j) if dx == 0 else None
                yield copy, me, src, dst

    def face_wait(m):
        dk, _, tiles, t0 = segs[m]
        own = (gz == 0) & (ring(gy, ny, dk) == 0)

        def take(count):
            dst = GB.at[pl.ds(t0, tiles), pl.ds(0, count), :]
            remote(dst, dst, face_send.at[0, m], face_recv.at[m], y_dev[0]).wait_recv()

        @pl.when(jnp.logical_not(own))
        def _():
            take(strip + 2 * SUB)

        @pl.when(own & ((gy == 0) | (gy == ny - 1)))
        def _():
            take(SUB)

    def wt_copy():
        where = pl.ds(pl.multiple_of(gy * strip, SUB), strip)
        return remote(WS, WR.at[:, where, :], wt_send, wt_recv.at[gy], dev(gx, gz, 0))

    for k in range(gt):
        load_gas(0, temp_in, k).start()
    load_flags.start()
    for c in range(chunks):
        for k in range(wt):
            load_wall(solid_in, c, k).start()
    for k in range(gt):
        load_gas(1, fuel_in, k).start()
    load_owner.start()
    for c in range(chunks):
        for k in range(wt):
            load_wall(diff_in, c, k).start()
    load_vel.start()

    for k in range(gt):
        load_gas(0, temp_in, k).wait()
    load_flags.wait()

    @pl.when(gz == 0)
    def _():
        for k in range(gt):
            on = FL[:, k * LANES : (k + 1) * LANES].astype(jnp.float32)
            GS[k] = on * G[0, 1, k, top : top + rows_g, :]
        for copy, me, src, dst in face_pieces():
            if me is None:
                copy.start()
            else:

                @pl.when(jnp.logical_not(me))
                def _(copy=copy):
                    copy.start()

                @pl.when(me)
                def _(src=src, dst=dst):
                    dst[...] = src[...]

    def send_first(i, carry):
        c = lax.rem(i + 1, chunks)
        for k in range(wt):
            load_wall(solid_in, c, k).wait()
        pack_rows(A, 0, c, units)
        for way in range(2):
            first_copy(c, way).start()
        return carry

    lax.fori_loop(0, chunks, send_first, 0)

    for k in range(gt):
        load_gas(1, fuel_in, k).wait()
    per = SUB // (2 * gt)

    def pack_x(i, carry):
        for way in range(2):
            for f in range(2):
                for n in range(per):
                    for k in range(gt):
                        z = i * per + n
                        at = (f * per + n) * gt + k
                        XS[way, i, at : at + 1, :] = G[f, z + 1, k, inner_g[way] : inner_g[way] + 1, :]
        return carry

    lax.fori_loop(0, layers_g // per, pack_x, 0)
    for way in range(2):
        x_copy(way).start()
    for f in range(2):
        for way in range(2):

            @pl.when(has_z[way])
            def _(f=f, way=way):
                z_copy(f, way).start()

        @pl.when(gz == 0)
        def _(f=f):
            for k in range(gt):
                G[f, 0, k, top : top + rows_g, :] = G[f, 1, k, top : top + rows_g, :]

        @pl.when(gz == nz - 1)
        def _(f=f):
            for k in range(gt):
                G[f, layers_g + 1, k, top : top + rows_g, :] = G[f, layers_g, k, top : top + rows_g, :]

    for c in range(chunks):
        for k in range(wt):
            load_wall(diff_in, c, k).wait()
    group = lane // GROUP
    within = lane % GROUP
    low_half = within < 2 * HALO

    def pack_edges(i, carry):
        c = lax.rem(i + 1, chunks)
        for r in range(rtiles):
            acc = jnp.zeros((SUB, LANES), jnp.float32)
            for l in range(CHUNK):
                far = (wt - 1) * CHUNK + l
                at = slice(top + r * SUB, top + (r + 1) * SUB)
                ad = slice(r * SUB, (r + 1) * SUB)
                s = jnp.where(lane >= LANES - HALO, A[c, far, at, :], A[c, l, at, :])
                d = jnp.where(lane >= LANES - HALO, D[c, far, ad, :], D[c, l, ad, :])
                s = pltpu.roll(s, GROUP * l + HALO, 1)
                d = pltpu.roll(d, (GROUP * l + 3 * HALO) % LANES, 1)
                acc = jnp.where(group == l, jnp.where(low_half, s, d), acc)
            E[c, r * SUB : (r + 1) * SUB, :] = acc
        for way in range(2):
            edge_copy(c, way).start()
        return carry

    lax.fori_loop(0, chunks, pack_edges, 0)

    load_owner.wait()
    all_cols, all_rows = cols_g * ny, rows_g * nx

    def wrapped(x, n):
        x = jnp.where(x < 0, x + n, x)
        return jnp.where(x >= n, x - n, x)

    for r in range(rtiles):
        rr = slice(r * SUB, (r + 1) * SUB)
        p = line * strip + (r * SUB + iota((SUB, LANES), 0)) // 2
        for k in range(wt):
            q = gz * cols_g + (k * LANES + lane) // 2
            owner = OW[rr, k * LANES : (k + 1) * LANES]
            if all_cols & (all_cols - 1) == 0:
                a = lax.shift_right_logical(owner, all_cols.bit_length() - 1)
                b = owner & (all_cols - 1)
            else:
                a = lax.div(owner, all_cols)
                b = owner - a * all_cols
            down = wrapped(a - p + DISP, all_rows)
            along = wrapped(b - q + DISP, all_cols)
            OW[rr, k * LANES : (k + 1) * LANES] = down * 16 + along
        first, final = OW[rr, 0:LANES], OW[rr, cols - LANES : cols]
        CO[rr, :] = pltpu.roll(jnp.where(lane >= LANES - HALO, final, first), HALO, 1)
    for way in range(2):
        code_copy(way).start()

    def pack_cols(i, acc):
        out = list(acc)
        for n in range(4):
            z = i * 4 + n
            for f in range(2):
                k = f * layers_g + z
                for r in range(gtiles):
                    at = slice(top + r * SUB, top + (r + 1) * SUB)
                    high = pltpu.roll(G[f, z + 1, gt - 1, at, :], k + 1, 1)
                    low = pltpu.roll(G[f, z + 1, 0, at, :], k + LANES // 2, 1)
                    new = jnp.where(lane == k, high, out[r])
                    out[r] = jnp.where(lane == k + LANES // 2, low, new)
        return tuple(out)

    zero = jnp.zeros((SUB, LANES), jnp.float32)
    packed = lax.fori_loop(0, layers_g // 4, pack_cols, (zero,) * gtiles)
    half = gtiles // 2
    left_half = lane < LANES // 2
    for r in range(half):
        rr = slice(r * SUB, (r + 1) * SUB)
        near, away = packed[r], packed[r + half]
        YS[0, rr, :] = jnp.where(left_half, near, pltpu.roll(away, LANES // 2, 1))
        YS[1, rr, :] = jnp.where(left_half, pltpu.roll(near, LANES // 2, 1), away)
    for way in range(2):
        y_copy(way).start()

    def build_zone(i, carry):
        c = lax.rem(i + 1, chunks)
        for way in range(2):
            edge_copy(c, way).wait_recv()
        for r in range(rtiles):
            rr = slice(r * SUB, (r + 1) * SUB)
            mine, left, right = E[c, rr, :], EN[0, c, rr, :], EN[1, c, rr, :]
            hi = (within < HALO) | ((within >= 2 * HALO) & (within < 3 * HALO))
            a = jnp.where(hi, left, mine)
            b = jnp.where(hi, mine, right)
            zone = jnp.where(low_half, a, pltpu.roll(b, 2 * HALO, 1))
            A[c, units, top + r * SUB : top + (r + 1) * SUB, :] = zone
            D[c, units, rr, :] = jnp.where(low_half, pltpu.roll(a, LANES - 2 * HALO, 1), b)
        for way in range(2):
            ZS[way, pl.ds(c, 1), :] = A[c, units, inner[way] : inner[way] + 1, :]
        return carry

    lax.fori_loop(0, chunks, build_zone, 0)
    for way in range(2):
        zone_copy(way).start()

    load_vel.wait()

    def wall_flux():
        for m in range(len(segs)):
            face_wait(m)
        for way in range(2):
            code_copy(way).wait_recv()
        back = LANES // 4
        for m in range(wt):
            start = LANES + m * (LANES // 2) - back
            a, off = start // LANES, start % LANES
            for r in range((strip + 2 * SUB) // SUB):
                rr = slice(r * SUB, (r + 1) * SUB)
                u = pltpu.roll(GB[a, rr, :], LANES - off, 1)
                v = pltpu.roll(GB[a + 1, rr, :], LANES - off, 1)
                w = jnp.where(lane < LANES - off, u, v)
                DW[m, pl.ds(2 * r * SUB, SUB, stride=2), :] = w
                DW[m, pl.ds(2 * r * SUB + 1, SUB, stride=2), :] = w

        def pick(r, code, windows):
            row, col = lax.shift_right_logical(code, 4), code & 15
            g = jnp.zeros((SUB, LANES), jnp.float32)
            for n in range(SPAN):
                got = None
                for mask, m, base in windows:
                    u = DW[m, r * SUB + 2 * n + 2 * (SUB - DISP) : r * SUB + 2 * n + 2 * (SUB - DISP) + SUB, :]
                    x = lanes_of(u, (base + col) & (LANES - 1))
                    got = x if got is None else jnp.where(mask, got, x)
                g = jnp.where(row == n, got, g)
            return g

        def flux_of(g, surf):
            power = jnp.exp(0.7 * jnp.log(jnp.maximum(g, 1.0)))
            film = jnp.where(g > 0.0, FILM_COEF * power, 0.0)
            return SOURCE_GAIN * film * (g - surf)

        for r in range(rtiles):
            rr = slice(r * SUB, (r + 1) * SUB)
            at = slice(top + r * SUB, top + (r + 1) * SUB)
            for m in range(wt):
                base = lane // 2 + back - DISP
                g = pick(r, OW[rr, m * LANES : (m + 1) * LANES], ((None, m, base),))
                F[m, rr, :] = flux_of(g, A[0, m * CHUNK, at, :])
            mine, left, right = CO[rr, :], CN[0, rr, :], CN[1, rr, :]
            near = lane < HALO
            a = jnp.where(near, left, mine)
            b = pltpu.roll(jnp.where(near, mine, right), 2 * HALO, 1)
            code = jnp.where(lane < 2 * HALO, a, b)
            lo = lane // 2 - HALO // 2 + back - DISP
            hi = lane // 2 - HALO + cols_g - HALO // 2 - ((wt - 1) * (LANES // 2) - back) - DISP
            g = pick(r, code, ((lane < 2 * HALO, 0, lo), (lane < 2 * HALO, wt - 1, hi)))
            flux = flux_of(g, A[0, units, at, :])
            F[wt, rr, :] = jnp.where(lane < GROUP, flux, 0.0)

    def gas_layer(z):
        gi = z + 1
        for r in range(gtiles):
            base = top + r * SUB
            at = slice(base, base + SUB)
            rr = slice(r * SUB, (r + 1) * SUB)
            shift = LANES // 2 if r >= half else 0
            fold = slice((r % half) * SUB, (r % half + 1) * SUB)
            rates = []
            for f in range(2):
                c = [G[f, gi, k, at, :] for k in range(gt)]
                key = f * layers_g + z + shift
                low = pltpu.roll(YR[0, fold, :], lax.rem(LANES - key, LANES), 1)
                high = pltpu.roll(YR[1, fold, :], LANES - 1 - key, 1)
                fwd = [low] + [pltpu.roll(x, 1, 1) for x in c]
                bwd = [pltpu.roll(x, LANES - 1, 1) for x in c] + [high]
                out = []
                for k in range(gt):
                    xl = G[f, gi, k, base - 1 : base - 1 + SUB, :]
                    xh = G[f, gi, k, base + 1 : base + 1 + SUB, :]
                    zl, zh = G[f, gi - 1, k, at, :], G[f, gi + 1, k, at, :]
                    yl = jnp.where(lane == 0, fwd[k], fwd[k + 1])
                    yh = jnp.where(lane == LANES - 1, bwd[k + 1], bwd[k])
                    cs = slice(k * LANES, (k + 1) * LANES)
                    advect = V[0, z, rr, cs] * (zh - zl) + V[1, z, rr, cs] * (xh - xl) + V[2, z, rr, cs] * (yh - yl)
                    nearby = zl + zh + xl + xh + yl + yh
                    coef = DIFFUSE_TEMP if f == 0 else DIFFUSE_FUEL
                    out.append((c[k], coef * (nearby - 6.0 * c[k]) - 0.5 * advect))
                rates.append(out)
            for k in range(gt):
                cs = slice(k * LANES, (k + 1) * LANES)
                (t, t_rate), (y, y_rate) = rates[0][k], rates[1][k]
                reaction = RATE_CONST * y * jnp.exp(-ACTIVATION / t)
                TO[z, rr, cs] = t + TIME_STEP * (t_rate + HEAT_RELEASE * reaction)
                FO[z, rr, cs] = y + TIME_STEP * (y_rate - reaction)

    def wall_chunk(src, dst, c):
        first, final = c == 0, c == chunks - 1
        cb, ca = jnp.maximum(c - 1, 0), jnp.minimum(c + 1, chunks - 1)
        lb = jnp.where(first, 0, CHUNK - 1)
        for r in range(rtiles):
            base = top + r * SUB
            at = slice(base, base + SUB)
            rr = slice(r * SUB, (r + 1) * SUB)
            zone = src[c, units, at, :]
            for l in range(CHUNK):
                cs = [src[c, k * CHUNK + l, at, :] for k in range(wt)]
                left = pltpu.roll(zone, LANES - GROUP * l - HALO + 1, 1)
                right = pltpu.roll(zone, LANES - 1 - GROUP * l - 3 * HALO, 1)
                fwd = [left] + [pltpu.roll(x, 1, 1) for x in cs]
                bwd = [pltpu.roll(x, LANES - 1, 1) for x in cs] + [right]
                for k in range(wt):
                    u = k * CHUNK + l
                    below = src[c, u - 1, at, :] if l else src[cb, k * CHUNK + lb, at, :]
                    if l < CHUNK - 1:
                        above = src[c, u + 1, at, :]
                    else:
                        above = jnp.where(final, COOLANT, src[ca, k * CHUNK, at, :])
                    nearby = below + above
                    nearby = nearby + src[c, u, base - 1 : base - 1 + SUB, :]
                    nearby = nearby + src[c, u, base + 1 : base + 1 + SUB, :]
                    nearby = nearby + jnp.where(lane == 0, fwd[k], fwd[k + 1])
                    nearby = nearby + jnp.where(lane == LANES - 1, bwd[k + 1], bwd[k])
                    dst[c, u, at, :] = cs[k] + D[c, u, rr, :] * (nearby - 6.0 * cs[k])
            below = jnp.where(first, zone, pltpu.roll(src[cb, units, at, :], GROUP, 1))
            below = jnp.where(lane < GROUP, below, pltpu.roll(zone, GROUP, 1))
            above = jnp.where(final, COOLANT, pltpu.roll(src[ca, units, at, :], LANES - GROUP, 1))
            above = jnp.where(lane >= LANES - GROUP, above, pltpu.roll(zone, LANES - GROUP, 1))
            nearby = below + above
            nearby = nearby + src[c, units, base - 1 : base - 1 + SUB, :]
            nearby = nearby + src[c, units, base + 1 : base + 1 + SUB, :]
            nearby = nearby + pltpu.roll(zone, 1, 1) + pltpu.roll(zone, LANES - 1, 1)
            dst[c, units, at, :] = zone + D[c, units, rr, :] * (nearby - 6.0 * zone)

        @pl.when(first)
        def _():
            for r in range(rtiles):
                at = slice(top + r * SUB, top + (r + 1) * SUB)
                rr = slice(r * SUB, (r + 1) * SUB)
                for k in range(wt):
                    dst[0, k * CHUNK, at, :] = dst[0, k * CHUNK, at, :] + F[k, rr, :]
                dst[0, units, at, :] = dst[0, units, at, :] + F[wt, rr, :]

    def step(src, dst, u, odd, i):
        t = 2 * u + 2 - odd
        s = (t - 1) * chunks + i
        c = lax.rem(i + 1, chunks)
        z = lax.rem(s + 1, layers_g)
        if odd:

            @pl.when(s == 0)
            def _():
                for way in range(2):
                    y_copy(way).wait_recv()
                    zone_copy(way).wait_recv()
                    x_copy(way).wait_recv()
                    for f in range(2):

                        @pl.when(has_z[1 - way])
                        def _(f=f, way=way):
                            z_copy(f, way).wait_recv()

                    for n in range(chunks):
                        A[n, units, outer[way] : outer[way] + 1, :] = ZR[way, n : n + 1, :]

                def unpack_x(j, carry):
                    for way in range(2):
                        for f in range(2):
                            for n in range(per):
                                for k in range(gt):
                                    at = (f * per + n) * gt + k
                                    G[f, j * per + n + 1, k, outer_g[way] : outer_g[way] + 1, :] = XR[
                                        way, j, at : at + 1, :
                                    ]
                    return carry

                lax.fori_loop(0, layers_g // per, unpack_x, 0)

        gas_layer(z)
        store_gas(1, z).start()

        @pl.when(z > 0)
        def _():
            store_gas(0, z).start()

        if odd:

            @pl.when(u == 0)
            def _():
                for way in range(2):
                    first_copy(c, way).wait_recv()
                unpack_rows(src, 0, c, units)

            @pl.when(u > 0)
            def _():
                for way in range(2):
                    row_copy(t - 1, c, way).wait_recv()
                unpack_rows(src, t - 1, c, units + 1)

            @pl.when((u == 0) & (c == 0))
            def _():
                wall_flux()

        else:
            for way in range(2):
                row_copy(t - 1, c, way).wait_recv()
            unpack_rows(src, t - 1, c, units + 1)

        wall_chunk(src, dst, c)

        def send():
            pack_rows(dst, t, c, units + 1)
            for way in range(2):
                row_copy(t, c, way).start()

        if odd:
            send()
        else:
            pl.when(t < SUBSTEPS)(send)

            @pl.when(t == SUBSTEPS)
            def _():
                for k in range(wt):
                    store_wall(c, k).start()

    def two_steps(u, carry):
        for odd, src, dst in ((1, A, B), (0, B, A)):

            def body(i, inner_carry, odd=odd, src=src, dst=dst):
                step(src, dst, u, odd, i)
                return inner_carry

            lax.fori_loop(0, chunks, body, 0)
        return carry

    lax.fori_loop(0, SUBSTEPS // 2, two_steps, 0)

    for r in range(strip // SUB):
        pairs = []
        for k in range(wt):
            base = top + 2 * r * SUB
            x = A[0, k * CHUNK, pl.ds(base, SUB, stride=2), :] + A[0, k * CHUNK, pl.ds(base + 1, SUB, stride=2), :]
            pairs.append(0.25 * (x + pltpu.roll(x, LANES - 1, 1)))
        idx = (2 * lane) & (LANES - 1)
        for k in range(gt):
            a, b = lanes_of(pairs[2 * k], idx), lanes_of(pairs[2 * k + 1], idx)
            WS[k, r * SUB : (r + 1) * SUB, :] = jnp.where(lane < LANES // 2, a, b)
    self_tile = (gz == 0) & (gy == 0)

    @pl.when(jnp.logical_not(self_tile))
    def _():
        wt_copy().start()

    @pl.when(self_tile)
    def _():
        WR[:, 0:strip, :] = WS[...]

    @pl.when(gz == 0)
    def _():
        for j in range(ny):
            where = pl.ds(j * strip, strip)

            def take(where=where, j=j):
                remote(WS, WR.at[:, where, :], wt_send, wt_recv.at[j], y_dev[0]).wait_recv()

            if j == 0:
                pl.when(gy > 0)(take)
            else:
                take()
        for k in range(gt):
            cs = slice(k * LANES, (k + 1) * LANES)
            gap = jnp.where(FL[:, cs] == 1, 2.0 * (WR[k] - G[0, 1, k, top : top + rows_g, :]), 0.0)
            TO[0, :, cs] = TO[0, :, cs] + TIME_STEP * (0.5 * V[0, 0, :, cs] + DIFFUSE_TEMP) * gap

    store_gas(0, 0).start()

    @pl.when(gz == 0)
    def _():
        for copy, me, _, _ in face_pieces():
            if me is None:
                copy.wait_send()
            else:
                pl.when(jnp.logical_not(me))(copy.wait_send)

    pl.when(jnp.logical_not(self_tile))(lambda: wt_copy().wait_send())
    for way in range(2):
        code_copy(way).wait_send()
        y_copy(way).wait_send()
        zone_copy(way).wait_send()
        x_copy(way).wait_send()
        for f in range(2):

            @pl.when(has_z[way])
            def _(f=f, way=way):
                z_copy(f, way).wait_send()

    def drain(c, carry):
        for way in range(2):
            edge_copy(c, way).wait_send()
            first_copy(c, way).wait_send()
            for t in range(1, SUBSTEPS):
                row_copy(t, c, way).wait_send()
        for k in range(wt):
            store_wall(c, k).wait()
        return carry

    lax.fori_loop(0, chunks, drain, 0)

    def drain_gas(z, carry):
        store_gas(0, z).wait()
        store_gas(1, z).wait()
        return carry

    lax.fori_loop(0, layers_g, drain_gas, 0)


def shards(mesh_shape, gas_temp, fuel_frac, velocity, wall_flags, solid_temp, diffusivity, gas_owner):
    nx, ny, nz = mesh_shape
    layers_g, rows_g, cols_g = gas_temp.shape
    layers, rows, cols = solid_temp.shape
    chunks, wt, gt = layers // CHUNK, cols // LANES, cols_g // LANES
    units = wt * CHUNK
    strip = rows // 2
    assert ny == nz and cols == 2 * cols_g and rows * ny == 2 * rows_g
    assert layers_g == SUBSTEPS * chunks and 2 * layers_g <= LANES // 2 and chunks * wt >= layers_g
    assert wt == 2 * gt and gt == 2 and layers % CHUNK == 0
    f32, i32 = jnp.float32, jnp.int32
    dma = pltpu.SemaphoreType.DMA
    scratch = [
        pltpu.VMEM((2, layers_g + 2, gt, rows_g + 2 * SUB, LANES), f32),
        pltpu.VMEM((3, layers_g, rows_g, cols_g), f32),
        pltpu.VMEM((rows_g, cols_g), i32),
        pltpu.VMEM((chunks, units + 1, rows + 2 * SUB, LANES), f32),
        pltpu.VMEM((chunks, units + 1, rows + 2 * SUB, LANES), f32),
        pltpu.VMEM((chunks, units + 1, rows, LANES), f32),
        pltpu.VMEM((layers_g, rows_g, cols_g), f32),
        pltpu.VMEM((layers_g, rows_g, cols_g), f32),
        pltpu.VMEM((rows, cols), i32),
        pltpu.VMEM((chunks, rows, LANES), f32),
        pltpu.VMEM((2, chunks, rows, LANES), f32),
        pltpu.VMEM((rows, LANES), i32),
        pltpu.VMEM((2, rows, LANES), i32),
        pltpu.VMEM((2, SUBSTEPS, chunks, units + SUB, LANES), f32),
        pltpu.VMEM((2, SUBSTEPS, chunks, units + SUB, LANES), f32),
        pltpu.VMEM((2, chunks, LANES), f32),
        pltpu.VMEM((2, chunks, LANES), f32),
        pltpu.VMEM((2, layers_g * 2 * gt // SUB, SUB, LANES), f32),
        pltpu.VMEM((2, layers_g * 2 * gt // SUB, SUB, LANES), f32),
        pltpu.VMEM((2, rows_g // 2, LANES), f32),
        pltpu.VMEM((2, rows_g // 2, LANES), f32),
        pltpu.VMEM((gt, rows_g, LANES), f32),
        pltpu.VMEM((gt + 2, strip + 2 * SUB, LANES), f32),
        pltpu.VMEM((wt, 2 * (strip + 2 * SUB), LANES), f32),
        pltpu.VMEM((wt + 1, rows, LANES), f32),
        pltpu.VMEM((gt, strip, LANES), f32),
        pltpu.VMEM((gt, rows_g, LANES), f32),
        dma((chunks, wt)),
        dma((chunks, wt)),
        dma((2, gt)),
        dma((3,)),
        dma((3, chunks, wt)),
        dma((2, SUBSTEPS, chunks)),
        dma((2, SUBSTEPS, chunks)),
        dma((2,)),
        dma((2,)),
        dma((2, chunks)),
        dma((2, chunks)),
        dma((2,)),
        dma((2,)),
        dma((2,)),
        dma((2,)),
        dma((2,)),
        dma((2,)),
        dma((2, 2)),
        dma((2, 2)),
        dma((ny + 2, 3)),
        dma((3,)),
        dma(()),
        dma((ny,)),
    ]
    return pl.pallas_call(
        functools.partial(mega_kernel, mesh_shape),
        out_shape=(
            jax.ShapeDtypeStruct(gas_temp.shape, f32),
            jax.ShapeDtypeStruct(fuel_frac.shape, f32),
            jax.ShapeDtypeStruct(solid_temp.shape, f32),
        ),
        in_specs=[ANY] * 7,
        out_specs=(ANY,) * 3,
        scratch_shapes=scratch,
        compiler_params=pltpu.CompilerParams(vmem_limit_bytes=60 << 20, has_side_effects=True),
        cost_estimate=pl.CostEstimate(flops=200_000_000, bytes_accessed=26 << 20, transcendentals=1 << 19),
        name="section",
    )(gas_temp, fuel_frac, velocity, wall_flags, solid_temp, diffusivity, gas_owner)


def solution(mesh):
    placed = (
        P("gz", "gx", "gy"),
        P("gz", "gx", "gy"),
        P(None, "gz", "gx", "gy"),
        P("gx", "gy"),
        P(None, ("gx", "gy"), "gz"),
        P(None, ("gx", "gy"), "gz"),
        P(("gx", "gy"), "gz"),
    )
    mesh_shape = tuple(mesh.shape[a] for a in ("gx", "gy", "gz"))
    return jax.shard_map(
        functools.partial(shards, mesh_shape),
        mesh=mesh,
        in_specs=placed,
        out_specs=(P("gz", "gx", "gy"), P("gz", "gx", "gy"), P(None, ("gx", "gy"), "gz")),
        check_vma=False,
    )
```

```python
import functools

import jax
import jax.numpy as jnp
from jax import lax
from jax.experimental import pallas as pl
from jax.experimental.pallas import tpu as pltpu
from jax.sharding import PartitionSpec as P

SUBSTEPS = 4
DISP = 4

FILM_COEF = 0.15
SOURCE_GAIN = 0.25
COOLANT = 1.0
DIFFUSE_TEMP = 0.2
DIFFUSE_FUEL = 0.15
TIME_STEP = 0.2
RATE_CONST = 1.0
ACTIVATION = 4.0
HEAT_RELEASE = 3.0

LANES = 128
SUB = 8
CHUNK = 8
GROUP = LANES // CHUNK
HALO = SUBSTEPS
SPAN = 2 * DISP + 1
PIECES = 4
MESH = pl.DeviceIdType.MESH
ANY = pl.BlockSpec(memory_space=pl.ANY)
VMEM = pl.BlockSpec(memory_space=pltpu.VMEM)


def iota(shape, dim):
    return lax.broadcasted_iota(jnp.int32, shape, dim)


def lanes_of(x, idx):
    return jnp.take_along_axis(x, idx, axis=1, mode="promise_in_bounds")


def mega_kernel(
    mesh_shape,
    temp_in,
    fuel_in,
    vel_in,
    flags_in,
    solid_in,
    diff_in,
    owner_in,
    TO,
    FO,
    SO,
    G,
    V,
    FL,
    A,
    B,
    D,
    OW,
    E,
    EN,
    CO,
    CN,
    MS,
    MR,
    ZS,
    ZR,
    XS,
    XR,
    YS,
    YR,
    GS,
    GB,
    DW,
    F,
    L0,
    WS,
    WR,
    load_s,
    load_d,
    load_g,
    load_m,
    row_send,
    row_recv,
    zone_send,
    zone_recv,
    edge_send,
    edge_recv,
    code_send,
    code_recv,
    y_send,
    y_recv,
    x_send,
    x_recv,
    z_send,
    z_recv,
    face_send,
    face_recv,
    wt_send,
    wt_recv,
):
    nx, ny, nz = mesh_shape
    gx, gy, gz = lax.axis_index("gx"), lax.axis_index("gy"), lax.axis_index("gz")
    layers_g, rows_g, cols_g = temp_in.shape
    layers, rows, cols = solid_in.shape
    chunks = layers // CHUNK
    wt = cols // LANES
    gt = cols_g // LANES
    units = wt * CHUNK
    strip = rows // 2
    top = SUB
    rtiles = rows // SUB
    gtiles = rows_g // SUB
    steps = SUBSTEPS * chunks
    lane = iota((SUB, LANES), 1)

    def dev(x, y, z):
        return (x, y, z)

    def ring(i, n, by):
        return lax.rem(i + n + by, n)

    line = gx * ny + gy
    line_next, line_prev = ring(line, nx * ny, 1), ring(line, nx * ny, -1)
    row_dev = (
        dev(lax.div(line_next, ny), lax.rem(line_next, ny), gz),
        dev(lax.div(line_prev, ny), lax.rem(line_prev, ny), gz),
    )
    col_dev = (dev(gx, gy, ring(gz, nz, 1)), dev(gx, gy, ring(gz, nz, -1)))
    y_dev = (dev(gx, ring(gy, ny, 1), gz), dev(gx, ring(gy, ny, -1), gz))
    x_dev = (dev(ring(gx, nx, 1), gy, gz), dev(ring(gx, nx, -1), gy, gz))

    def remote(src, dst, ssem, rsem, to):
        return pltpu.make_async_remote_copy(
            src_ref=src, dst_ref=dst, send_sem=ssem, recv_sem=rsem, device_id=to, device_id_type=MESH
        )

    def load_gas(f, src, k):
        return pltpu.make_async_copy(
            src.at[:, :, pl.ds(k * LANES, LANES)],
            G.at[f, pl.ds(1, layers_g), k, pl.ds(top, rows_g), :],
            load_g.at[f, k],
        )

    def load_wall(src, c, k):
        if src is solid_in:
            dst = A.at[c, pl.ds(k * CHUNK, CHUNK), pl.ds(top, rows), :]
            sem = load_s.at[c, k]
        else:
            dst = D.at[c, pl.ds(k * CHUNK, CHUNK), :, :]
            sem = load_d.at[c, k]
        return pltpu.make_async_copy(src.at[pl.ds(c * CHUNK, CHUNK), :, pl.ds(k * LANES, LANES)], dst, sem)

    load_flags = pltpu.make_async_copy(flags_in, FL, load_m.at[0])
    load_owner = pltpu.make_async_copy(owner_in, OW, load_m.at[1])
    load_vel = pltpu.make_async_copy(vel_in, V, load_m.at[2])

    def row_copy(t, c, way):
        count = pl.ds(0, units + 1)
        return remote(
            MS.at[way, t, c, count, :],
            MR.at[way, t, c, count, :],
            row_send.at[way, t, c],
            row_recv.at[way, t, c],
            row_dev[way],
        )

    def first_copy(c, way):
        count = pl.ds(0, units)
        return remote(
            MS.at[way, 0, c, count, :],
            MR.at[way, 0, c, count, :],
            row_send.at[way, 0, c],
            row_recv.at[way, 0, c],
            row_dev[way],
        )

    diag_dev = tuple(
        tuple(dev(x, y, ring(gz, nz, by)) for by in (1, 0, -1)) for x, y, _ in row_dev
    )

    def zone_copy(way, n):
        return remote(ZS.at[way], ZR.at[way, n], zone_send.at[way, n], zone_recv.at[way, n], diag_dev[way][n])

    inner = ((top + rows - 1), top)
    outer = ((top - 1), top + rows)

    tall = rows + 2 * SUB
    flat_a, flat_b = (x.reshape(chunks * (units + 1) * tall, LANES) for x in (A, B))

    def column(c, k, row):
        return pl.ds((c * (units + 1) + k * CHUNK) * tall + row, CHUNK, stride=tall)

    def pack_rows(src, t, c, zone):
        for way in range(2):
            for k in range(wt):
                MS[way, t, c, k * CHUNK : (k + 1) * CHUNK, :] = (flat_a if src is A else flat_b)[column(c, k, inner[way]), :]
            if zone:
                MS[way, t, c, units : units + 1, :] = src[c, units, inner[way] : inner[way] + 1, :]

    def unpack_rows(dst, t, c, zone):
        for way in range(2):
            for k in range(wt):
                (flat_a if dst is A else flat_b)[column(c, k, outer[way]), :] = MR[way, t, c, k * CHUNK : (k + 1) * CHUNK, :]
            if zone:
                dst[c, units, outer[way] : outer[way] + 1, :] = MR[way, t, c, units : units + 1, :]

    def edge_copy(c, way):
        return remote(E.at[c], EN.at[way, c], edge_send.at[way, c], edge_recv.at[way, c], col_dev[way])

    def code_copy(way):
        return remote(CO, CN.at[way], code_send.at[way], code_recv.at[way], col_dev[way])

    def y_copy(way):
        return remote(YS.at[way], YR.at[way], y_send.at[way], y_recv.at[way], y_dev[way])

    def x_copy(way):
        return remote(XS.at[way], XR.at[way], x_send.at[way], x_recv.at[way], x_dev[way])

    inner_g = (top + rows_g - 1, top)
    outer_g = (top - 1, top + rows_g)

    def z_copy(f, way):
        src, dst = ((layers_g, 0), (1, layers_g + 1))[way]
        return remote(
            G.at[f, src, :, pl.ds(top, rows_g), :],
            G.at[f, dst, :, pl.ds(top, rows_g), :],
            z_send.at[f, way],
            z_recv.at[f, way],
            col_dev[way],
        )

    has_z = (gz < nz - 1, gz > 0)

    segs = (
        (0, 0, gt, 1),
        (1, gt - 1, 1, 0),
        (-1, 0, 1, gt + 1),
    )
    parts = []
    for j in range(ny):
        r0, r1 = max(0, strip * j - DISP), min(rows_g, strip * (j + 1) + DISP)
        parts.append((0, j, r0, r1 - r0, r0 - (strip * j - DISP)))
    parts.append((1, 0, rows_g - DISP, DISP, 0))
    parts.append((-1, ny - 1, 0, DISP, strip + DISP))

    def face_pieces():
        for n, (dx, j, r0, count, d0) in enumerate(parts):
            for m, (dk, s0, tiles, t0) in enumerate(segs):
                k = ring(gy, ny, dk)
                src = GS.at[pl.ds(s0, tiles), pl.ds(r0, count), :]
                dst = GB.at[pl.ds(t0, tiles), pl.ds(d0, count), :]
                copy = remote(src, dst, face_send.at[n, m], face_recv.at[m], dev(ring(gx, nx, dx), j, k))
                me = (k == 0) & (gy == j) if dx == 0 else None
                yield copy, me, src, dst

    def face_wait(m):
        dk, _, tiles, t0 = segs[m]
        own = (gz == 0) & (ring(gy, ny, dk) == 0)

        def take(count):
            dst = GB.at[pl.ds(t0, tiles), pl.ds(0, count), :]
            remote(dst, dst, face_send.at[0, m], face_recv.at[m], y_dev[0]).wait_recv()

        @pl.when(jnp.logical_not(own))
        def _():
            take(strip + 2 * DISP)

        @pl.when(own & ((gy == 0) | (gy == ny - 1)))
        def _():
            take(DISP)

    def wt_copy():
        where = pl.ds(pl.multiple_of(gy * strip, SUB), strip)
        return remote(WS, WR.at[:, where, :], wt_send, wt_recv.at[gy], dev(gx, gz, 0))

    def load_face(k):
        return pltpu.make_async_copy(temp_in.at[0, :, pl.ds(k * LANES, LANES)], GS.at[k], load_m.at[3 + k])

    def start_wall(src):
        def body(i, carry):
            c = lax.rem(i + 1, chunks)
            for k in range(wt):
                load_wall(src, c, k).start()
            return carry

        lax.fori_loop(0, chunks, body, 0)

    barrier = pltpu.get_barrier_semaphore()

    def greet(to):
        pl.semaphore_signal(barrier, inc=1, device_id=to, device_id_type=MESH)

    for pair in (row_dev, col_dev, y_dev, x_dev):
        for to in pair:
            greet(to)
    for x, _, y in diag_dev:
        greet(x)
        greet(y)
    for dk in (0, 1, -1):
        k = ring(gz, ny, -dk)
        for dx, ask in ((0, None), (1, gy == ny - 1), (-1, gy == 0)):
            to = dev(ring(gx, nx, dx), k, 0)
            if dx == 0:
                ask = jnp.logical_not((gz == 0) & (gy == k))
            pl.when(ask)(functools.partial(greet, to))
    self_tile = (gz == 0) & (gy == 0)

    @pl.when(gz == 0)
    def _():
        for j in range(ny):
            pl.when(jnp.logical_not((gy == 0) & (j == 0)))(functools.partial(greet, dev(gx, j, gy)))

    load_flags.start()
    for k in range(gt):
        load_face(k).start()
    load_owner.start()
    start_wall(solid_in)
    start_wall(diff_in)
    for k in range(gt):
        load_gas(0, temp_in, k).start()
    for k in range(gt):
        load_gas(1, fuel_in, k).start()
    load_vel.start()

    load_flags.wait()
    for k in range(gt):
        load_face(k).wait()
        GS[k] = GS[k] * FL[:, k * LANES : (k + 1) * LANES].astype(jnp.float32)

    def pack_first(i, carry):
        c = lax.rem(i + 1, chunks)
        for k in range(wt):
            load_wall(solid_in, c, k).wait()
        pack_rows(A, 0, c, False)
        return carry

    lax.fori_loop(0, chunks, pack_first, 0)
    group = lane // GROUP
    within = lane % GROUP
    low_half = within < 2 * HALO

    def pack_edges(i, carry):
        c = i
        for k in range(wt):
            load_wall(diff_in, c, k).wait()
        for r in range(rtiles):
            acc = jnp.zeros((SUB, LANES), jnp.float32)
            for l in range(CHUNK):
                far = (wt - 1) * CHUNK + l
                at = slice(top + r * SUB, top + (r + 1) * SUB)
                ad = slice(r * SUB, (r + 1) * SUB)
                s = jnp.where(lane >= LANES - HALO, A[c, far, at, :], A[c, l, at, :])
                d = jnp.where(lane >= LANES - HALO, D[c, far, ad, :], D[c, l, ad, :])
                s = pltpu.roll(s, GROUP * l + HALO, 1)
                d = pltpu.roll(d, (GROUP * l + 3 * HALO) % LANES, 1)
                acc = jnp.where(group == l, jnp.where(low_half, s, d), acc)
            E[c, r * SUB : (r + 1) * SUB, :] = acc
        for way, row in ((0, rows - 1), (1, 0)):
            ZS[way, pl.ds(c, 1), :] = E[c, row : row + 1, :]
        return carry

    lax.fori_loop(0, chunks, pack_edges, 0)

    load_owner.wait()
    all_cols, all_rows = cols_g * ny, rows_g * nx

    def wrapped(x, n):
        x = jnp.where(x < 0, x + n, x)
        return jnp.where(x >= n, x - n, x)

    for r in range(rtiles):
        rr = slice(r * SUB, (r + 1) * SUB)
        p = line * strip + (r * SUB + iota((SUB, LANES), 0)) // 2
        for k in range(wt):
            q = gz * cols_g + (k * LANES + lane) // 2
            owner = OW[rr, k * LANES : (k + 1) * LANES]
            if all_cols & (all_cols - 1) == 0:
                a = lax.shift_right_logical(owner, all_cols.bit_length() - 1)
                b = owner & (all_cols - 1)
            else:
                a = lax.div(owner, all_cols)
                b = owner - a * all_cols
            down = wrapped(a - p + DISP, all_rows)
            along = wrapped(b - q + DISP, all_cols)
            OW[rr, k * LANES : (k + 1) * LANES] = down * 16 + along
        first, final = OW[rr, 0:LANES], OW[rr, cols - LANES : cols]
        CO[rr, :] = pltpu.roll(jnp.where(lane >= LANES - HALO, final, first), HALO, 1)

    mine = (gy == 0) | (gy == 1) | (gy == ny - 1)
    greeted = 12 + jnp.where(self_tile, 0, 1) + jnp.where(gz == 0, jnp.where(mine, 3 * ny + 5, 3 * ny + 6), 0)
    pl.semaphore_wait(barrier, greeted)

    def send_edges(c, carry):
        for way in range(2):
            edge_copy(c, way).start()
        return carry

    lax.fori_loop(0, chunks, send_edges, 0)
    for way in range(2):
        for n in range(3):
            zone_copy(way, n).start()
        code_copy(way).start()

    def send_first(i, carry):
        c = lax.rem(i + 1, chunks)
        for way in range(2):
            first_copy(c, way).start()
        return carry

    lax.fori_loop(0, chunks // 2, send_first, 0)

    @pl.when(gz == 0)
    def _():
        for copy, me, src, dst in face_pieces():
            if me is None:
                copy.start()
            else:

                @pl.when(jnp.logical_not(me))
                def _(copy=copy):
                    copy.start()

                @pl.when(me)
                def _(src=src, dst=dst):
                    dst[...] = src[...]

    lax.fori_loop(chunks // 2, chunks, send_first, 0)

    for k in range(gt):
        load_gas(0, temp_in, k).wait()
        load_gas(1, fuel_in, k).wait()
    per = SUB // (2 * gt)

    def pack_x(i, carry):
        for way in range(2):
            for f in range(2):
                for n in range(per):
                    for k in range(gt):
                        z = i * per + n
                        at = (f * per + n) * gt + k
                        XS[way, i, at : at + 1, :] = G[f, z + 1, k, inner_g[way] : inner_g[way] + 1, :]
        return carry

    lax.fori_loop(0, layers_g // per, pack_x, 0)
    for way in range(2):
        x_copy(way).start()
    for f in range(2):
        for way in range(2):

            @pl.when(has_z[way])
            def _(f=f, way=way):
                z_copy(f, way).start()

        @pl.when(gz == 0)
        def _(f=f):
            for k in range(gt):
                G[f, 0, k, top : top + rows_g, :] = G[f, 1, k, top : top + rows_g, :]

        @pl.when(gz == nz - 1)
        def _(f=f):
            for k in range(gt):
                G[f, layers_g + 1, k, top : top + rows_g, :] = G[f, layers_g, k, top : top + rows_g, :]

    def pack_cols(i, acc):
        out = list(acc)
        for n in range(4):
            z = i * 4 + n
            for f in range(2):
                k = f * layers_g + z
                for r in range(gtiles):
                    at = slice(top + r * SUB, top + (r + 1) * SUB)
                    high = pltpu.roll(G[f, z + 1, gt - 1, at, :], k + 1, 1)
                    low = pltpu.roll(G[f, z + 1, 0, at, :], k + LANES // 2, 1)
                    new = jnp.where(lane == k, high, out[r])
                    out[r] = jnp.where(lane == k + LANES // 2, low, new)
        return tuple(out)

    zero = jnp.zeros((SUB, LANES), jnp.float32)
    packed = lax.fori_loop(0, layers_g // 4, pack_cols, (zero,) * gtiles)
    half = gtiles // 2
    left_half = lane < LANES // 2
    for r in range(half):
        rr = slice(r * SUB, (r + 1) * SUB)
        near, away = packed[r], packed[r + half]
        YS[0, rr, :] = jnp.where(left_half, near, pltpu.roll(away, LANES // 2, 1))
        YS[1, rr, :] = jnp.where(left_half, pltpu.roll(near, LANES // 2, 1), away)
    for way in range(2):
        y_copy(way).start()

    hi = (within < HALO) | ((within >= 2 * HALO) & (within < 3 * HALO))

    def zone_of(mine, left, right):
        a = jnp.where(hi, left, mine)
        b = jnp.where(hi, mine, right)
        state = jnp.where(low_half, a, pltpu.roll(b, 2 * HALO, 1))
        return state, jnp.where(low_half, pltpu.roll(a, LANES - 2 * HALO, 1), b)

    def build_zone(c):
        for way in range(2):
            edge_copy(c, way).wait_recv()
        for r in range(rtiles):
            rr = slice(r * SUB, (r + 1) * SUB)
            state, coef = zone_of(E[c, rr, :], EN[0, c, rr, :], EN[1, c, rr, :])
            A[c, units, top + r * SUB : top + (r + 1) * SUB, :] = state
            D[c, units, rr, :] = coef

    def zone_rows():
        for way in range(2):
            for n in range(3):
                zone_copy(way, n).wait_recv()
            state, _ = zone_of(ZR[way, 1], ZR[way, 0], ZR[way, 2])
            ZR[way, 1] = state
            for n in range(chunks):
                A[n, units, outer[way] : outer[way] + 1, :] = ZR[way, 1, n : n + 1, :]

    def wall_flux():
        for m in range(len(segs)):
            face_wait(m)
        for way in range(2):
            code_copy(way).wait_recv()
        back = LANES // 4
        for m in range(wt):
            start = LANES + m * (LANES // 2) - back
            a, off = start // LANES, start % LANES
            for r in range((strip + 2 * DISP) // SUB):
                rr = slice(r * SUB, (r + 1) * SUB)
                u = pltpu.roll(GB[a, rr, :], LANES - off, 1)
                v = pltpu.roll(GB[a + 1, rr, :], LANES - off, 1)
                w = jnp.where(lane < LANES - off, u, v)
                DW[m, pl.ds(2 * r * SUB, SUB, stride=2), :] = w
                DW[m, pl.ds(2 * r * SUB + 1, SUB, stride=2), :] = w

        def pick(r, code, windows):
            row, col = lax.shift_right_logical(code, 4), code & 15
            g = jnp.zeros((SUB, LANES), jnp.float32)
            for n in range(SPAN):
                got = None
                for mask, m, base in windows:
                    u = DW[m, r * SUB + 2 * n : r * SUB + 2 * n + SUB, :]
                    x = lanes_of(u, (base + col) & (LANES - 1))
                    got = x if got is None else jnp.where(mask, got, x)
                g = jnp.where(row == n, got, g)
            return g

        def flux_of(g, surf):
            power = jnp.exp(0.7 * jnp.log(jnp.maximum(g, 1.0)))
            film = jnp.where(g > 0.0, FILM_COEF * power, 0.0)
            return SOURCE_GAIN * film * (g - surf)

        for r in range(rtiles):
            rr = slice(r * SUB, (r + 1) * SUB)
            at = slice(top + r * SUB, top + (r + 1) * SUB)
            for m in range(wt):
                base = lane // 2 + back - DISP
                g = pick(r, OW[rr, m * LANES : (m + 1) * LANES], ((None, m, base),))
                F[m, rr, :] = flux_of(g, A[0, m * CHUNK, at, :])
            mine, left, right = CO[rr, :], CN[0, rr, :], CN[1, rr, :]
            near = lane < HALO
            a = jnp.where(near, left, mine)
            b = pltpu.roll(jnp.where(near, mine, right), 2 * HALO, 1)
            code = jnp.where(lane < 2 * HALO, a, b)
            lo = lane // 2 - HALO // 2 + back - DISP
            hi = lane // 2 - HALO + cols_g - HALO // 2 - ((wt - 1) * (LANES // 2) - back) - DISP
            g = pick(r, code, ((lane < 2 * HALO, 0, lo), (lane < 2 * HALO, wt - 1, hi)))
            flux = flux_of(g, A[0, units, at, :])
            F[wt, rr, :] = jnp.where(lane < GROUP, flux, 0.0)

    def gas_layer(z):
        gi = z + 1
        for r in range(gtiles):
            base = top + r * SUB
            at = slice(base, base + SUB)
            rr = slice(r * SUB, (r + 1) * SUB)
            shift = LANES // 2 if r >= half else 0
            fold = slice((r % half) * SUB, (r % half + 1) * SUB)
            rates = []
            for f in range(2):
                c = [G[f, gi, k, at, :] for k in range(gt)]
                key = f * layers_g + z + shift
                low = pltpu.roll(YR[0, fold, :], lax.rem(LANES - key, LANES), 1)
                high = pltpu.roll(YR[1, fold, :], LANES - 1 - key, 1)
                fwd = [low] + [pltpu.roll(x, 1, 1) for x in c]
                bwd = [pltpu.roll(x, LANES - 1, 1) for x in c] + [high]
                out = []
                for k in range(gt):
                    xl = G[f, gi, k, base - 1 : base - 1 + SUB, :]
                    xh = G[f, gi, k, base + 1 : base + 1 + SUB, :]
                    zl, zh = G[f, gi - 1, k, at, :], G[f, gi + 1, k, at, :]
                    yl = jnp.where(lane == 0, fwd[k], fwd[k + 1])
                    yh = jnp.where(lane == LANES - 1, bwd[k + 1], bwd[k])
                    cs = slice(k * LANES, (k + 1) * LANES)
                    advect = V[0, z, rr, cs] * (zh - zl) + V[1, z, rr, cs] * (xh - xl) + V[2, z, rr, cs] * (yh - yl)
                    nearby = zl + zh + xl + xh + yl + yh
                    coef = DIFFUSE_TEMP if f == 0 else DIFFUSE_FUEL
                    out.append((c[k], coef * (nearby - 6.0 * c[k]) - 0.5 * advect))
                rates.append(out)
            for k in range(gt):
                cs = slice(k * LANES, (k + 1) * LANES)
                (t, t_rate), (y, y_rate) = rates[0][k], rates[1][k]
                reaction = RATE_CONST * y * jnp.exp(-ACTIVATION / t)
                TO[z, rr, cs] = t + TIME_STEP * (t_rate + HEAT_RELEASE * reaction)
                FO[z, rr, cs] = y + TIME_STEP * (y_rate - reaction)

    def wall_chunk(src, dst, c, last, tiles):
        first, final = c == 0, c == chunks - 1
        cb, ca = jnp.maximum(c - 1, 0), jnp.minimum(c + 1, chunks - 1)
        lb = jnp.where(first, 0, CHUNK - 1)
        for r in tiles:
            base = top + r * SUB
            at = slice(base, base + SUB)
            rr = slice(r * SUB, (r + 1) * SUB)
            zone = src[c, units, at, :]
            for l in range(CHUNK):
                cs = [src[c, k * CHUNK + l, at, :] for k in range(wt)]
                left = pltpu.roll(zone, LANES - GROUP * l - HALO + 1, 1)
                right = pltpu.roll(zone, LANES - 1 - GROUP * l - 3 * HALO, 1)
                fwd = [left] + [pltpu.roll(x, 1, 1) for x in cs]
                bwd = [pltpu.roll(x, LANES - 1, 1) for x in cs] + [right]
                for k in range(wt):
                    u = k * CHUNK + l
                    below = src[c, u - 1, at, :] if l else src[cb, k * CHUNK + lb, at, :]
                    if l < CHUNK - 1:
                        above = src[c, u + 1, at, :]
                    else:
                        above = jnp.where(final, COOLANT, src[ca, k * CHUNK, at, :])
                    nearby = below + above
                    nearby = nearby + src[c, u, base - 1 : base - 1 + SUB, :]
                    nearby = nearby + src[c, u, base + 1 : base + 1 + SUB, :]
                    nearby = nearby + jnp.where(lane == 0, fwd[k], fwd[k + 1])
                    nearby = nearby + jnp.where(lane == LANES - 1, bwd[k + 1], bwd[k])
                    new = cs[k] + D[c, u, rr, :] * (nearby - 6.0 * cs[k])
                    if last:
                        SO[c * CHUNK + l, rr, k * LANES : (k + 1) * LANES] = new
                    else:
                        dst[c, u, at, :] = new
            if last:
                continue
            below = jnp.where(first, zone, pltpu.roll(src[cb, units, at, :], GROUP, 1))
            below = jnp.where(lane < GROUP, below, pltpu.roll(zone, GROUP, 1))
            above = jnp.where(final, COOLANT, pltpu.roll(src[ca, units, at, :], LANES - GROUP, 1))
            above = jnp.where(lane >= LANES - GROUP, above, pltpu.roll(zone, LANES - GROUP, 1))
            nearby = below + above
            nearby = nearby + src[c, units, base - 1 : base - 1 + SUB, :]
            nearby = nearby + src[c, units, base + 1 : base + 1 + SUB, :]
            nearby = nearby + pltpu.roll(zone, 1, 1) + pltpu.roll(zone, LANES - 1, 1)
            dst[c, units, at, :] = zone + D[c, units, rr, :] * (nearby - 6.0 * zone)

        @pl.when(first)
        def _():
            for r in tiles:
                at = slice(top + r * SUB, top + (r + 1) * SUB)
                rr = slice(r * SUB, (r + 1) * SUB)
                for k in range(wt):
                    if last:
                        cs = slice(k * LANES, (k + 1) * LANES)
                        new = SO[0, rr, cs] + F[k, rr, :]
                        SO[0, rr, cs] = new
                        L0[k, rr, :] = new
                    else:
                        dst[0, k * CHUNK, at, :] = dst[0, k * CHUNK, at, :] + F[k, rr, :]
                if not last:
                    dst[0, units, at, :] = dst[0, units, at, :] + F[wt, rr, :]

    def gas_edges():
        load_vel.wait()
        for way in range(2):
            y_copy(way).wait_recv()
            x_copy(way).wait_recv()
            for f in range(2):

                @pl.when(has_z[1 - way])
                def _(f=f, way=way):
                    z_copy(f, way).wait_recv()

        def unpack_x(j, carry):
            for way in range(2):
                for f in range(2):
                    for n in range(per):
                        for k in range(gt):
                            at = (f * per + n) * gt + k
                            G[f, j * per + n + 1, k, outer_g[way] : outer_g[way] + 1, :] = XR[
                                way, j, at : at + 1, :
                            ]
            return carry

        lax.fori_loop(0, layers_g // per, unpack_x, 0)

    def wall_mean():
        for r in range(strip // SUB):
            pairs = []
            for k in range(wt):
                base = 2 * r * SUB
                x = L0[k, pl.ds(base, SUB, stride=2), :] + L0[k, pl.ds(base + 1, SUB, stride=2), :]
                pairs.append(0.25 * (x + pltpu.roll(x, LANES - 1, 1)))
            idx = (2 * lane) & (LANES - 1)
            for k in range(gt):
                a, b = lanes_of(pairs[2 * k], idx), lanes_of(pairs[2 * k + 1], idx)
                WS[k, r * SUB : (r + 1) * SUB, :] = jnp.where(lane < LANES // 2, a, b)

        @pl.when(jnp.logical_not(self_tile))
        def _():
            wt_copy().start()

        @pl.when(self_tile)
        def _():
            WR[:, 0:strip, :] = WS[...]

    surface_at = tuple(chunks - 2 - 2 * t for t in range(SUBSTEPS))
    gas_at = (0, 1, 2, 1)

    def step(src, dst, t, i):
        at = surface_at[t - 1]
        c = jnp.where(i < at, i + 1, jnp.where(i == at, 0, i))
        if t == 1:

            @pl.when(i == 0)
            def _():
                for n in range(3):
                    build_zone(n)
                zone_rows()

            @pl.when((c > 1) & (c < chunks - 1))
            def _():
                build_zone(c + 1)

        if t == 2:
            pl.when(i == 0)(gas_edges)
        for n in range(gas_at[t - 1]):
            done = sum(gas_at[: t - 1]) * chunks + i * gas_at[t - 1] + n
            gas_layer(lax.rem(done + 1, layers_g))
        for way in range(2):
            (first_copy(c, way) if t == 1 else row_copy(t - 1, c, way)).wait_recv()
        unpack_rows(src, t - 1, c, t > 1)
        if t == 1:
            pl.when(c == 0)(wall_flux)
        if t < SUBSTEPS:
            wall_chunk(src, dst, c, False, (0, rtiles - 1))
            pack_rows(dst, t, c, True)
            for way in range(2):
                row_copy(t, c, way).start()
            wall_chunk(src, dst, c, False, tuple(range(1, rtiles - 1)))
        else:
            wall_chunk(src, dst, c, True, tuple(range(rtiles)))
            pl.when(c == 0)(wall_mean)

    for t in range(1, SUBSTEPS + 1):
        src, dst = (A, B) if t % 2 else (B, A)

        def body(i, carry, src=src, dst=dst, t=t):
            step(src, dst, t, i)
            return carry

        lax.fori_loop(0, chunks, body, 0)

    @pl.when(gz == 0)
    def _():
        for j in range(ny):
            where = pl.ds(j * strip, strip)

            def take(where=where, j=j):
                remote(WS, WR.at[:, where, :], wt_send, wt_recv.at[j], y_dev[0]).wait_recv()

            if j == 0:
                pl.when(gy > 0)(take)
            else:
                take()
        for k in range(gt):
            cs = slice(k * LANES, (k + 1) * LANES)
            gap = jnp.where(FL[:, cs] == 1, 2.0 * (WR[k] - G[0, 1, k, top : top + rows_g, :]), 0.0)
            TO[0, :, cs] = TO[0, :, cs] + TIME_STEP * (0.5 * V[0, 0, :, cs] + DIFFUSE_TEMP) * gap

    @pl.when(gz == 0)
    def _():
        for copy, me, _, _ in face_pieces():
            if me is None:
                copy.wait_send()
            else:
                pl.when(jnp.logical_not(me))(copy.wait_send)

    pl.when(jnp.logical_not(self_tile))(lambda: wt_copy().wait_send())
    for way in range(2):
        code_copy(way).wait_send()
        y_copy(way).wait_send()
        for n in range(3):
            zone_copy(way, n).wait_send()
        x_copy(way).wait_send()
        for f in range(2):

            @pl.when(has_z[way])
            def _(f=f, way=way):
                z_copy(f, way).wait_send()

    def drain(c, carry):
        for way in range(2):
            edge_copy(c, way).wait_send()
            first_copy(c, way).wait_send()
            for t in range(1, SUBSTEPS):
                row_copy(t, c, way).wait_send()
        return carry

    lax.fori_loop(0, chunks, drain, 0)


def store_kernel(t_in, f_in, s_in, t_out, f_out, s_out, sems):
    copies = []
    for n, (src, dst) in enumerate(((s_in, s_out), (t_in, t_out), (f_in, f_out))):
        size = src.shape[0] // PIECES
        for m in range(PIECES):
            at = pl.ds(m * size, size)
            copies.append(pltpu.make_async_copy(src.at[at], dst.at[at], sems.at[n, m]))
    for copy in copies:
        copy.start()
    for copy in copies:
        copy.wait()


def shards(mesh_shape, gas_temp, fuel_frac, velocity, wall_flags, solid_temp, diffusivity, gas_owner):
    nx, ny, nz = mesh_shape
    layers_g, rows_g, cols_g = gas_temp.shape
    layers, rows, cols = solid_temp.shape
    chunks, wt, gt = layers // CHUNK, cols // LANES, cols_g // LANES
    units = wt * CHUNK
    strip = rows // 2
    assert ny == nz and cols == 2 * cols_g and rows * ny == 2 * rows_g
    assert layers_g == 4 * chunks and chunks == SUB and 2 * layers_g <= LANES // 2
    assert wt == 2 * gt and gt == 2 and layers % CHUNK == 0
    f32, i32 = jnp.float32, jnp.int32
    dma = pltpu.SemaphoreType.DMA
    scratch = [
        pltpu.VMEM((2, layers_g + 2, gt, rows_g + 2 * SUB, LANES), f32),
        pltpu.VMEM((3, layers_g, rows_g, cols_g), f32),
        pltpu.VMEM((rows_g, cols_g), i32),
        pltpu.VMEM((chunks, units + 1, rows + 2 * SUB, LANES), f32),
        pltpu.VMEM((chunks, units + 1, rows + 2 * SUB, LANES), f32),
        pltpu.VMEM((chunks, units + 1, rows, LANES), f32),
        pltpu.VMEM((rows, cols), i32),
        pltpu.VMEM((chunks, rows, LANES), f32),
        pltpu.VMEM((2, chunks, rows, LANES), f32),
        pltpu.VMEM((rows, LANES), i32),
        pltpu.VMEM((2, rows, LANES), i32),
        pltpu.VMEM((2, SUBSTEPS, chunks, units + SUB, LANES), f32),
        pltpu.VMEM((2, SUBSTEPS, chunks, units + SUB, LANES), f32),
        pltpu.VMEM((2, chunks, LANES), f32),
        pltpu.VMEM((2, 3, chunks, LANES), f32),
        pltpu.VMEM((2, layers_g * 2 * gt // SUB, SUB, LANES), f32),
        pltpu.VMEM((2, layers_g * 2 * gt // SUB, SUB, LANES), f32),
        pltpu.VMEM((2, rows_g // 2, LANES), f32),
        pltpu.VMEM((2, rows_g // 2, LANES), f32),
        pltpu.VMEM((gt, rows_g, LANES), f32),
        pltpu.VMEM((gt + 2, strip + 2 * DISP, LANES), f32),
        pltpu.VMEM((wt, 2 * (strip + 2 * DISP), LANES), f32),
        pltpu.VMEM((wt + 1, rows, LANES), f32),
        pltpu.VMEM((wt, rows, LANES), f32),
        pltpu.VMEM((gt, strip, LANES), f32),
        pltpu.VMEM((gt, rows_g, LANES), f32),
        dma((chunks, wt)),
        dma((chunks, wt)),
        dma((2, gt)),
        dma((3 + gt,)),
        dma((2, SUBSTEPS, chunks)),
        dma((2, SUBSTEPS, chunks)),
        dma((2, 3)),
        dma((2, 3)),
        dma((2, chunks)),
        dma((2, chunks)),
        dma((2,)),
        dma((2,)),
        dma((2,)),
        dma((2,)),
        dma((2,)),
        dma((2,)),
        dma((2, 2)),
        dma((2, 2)),
        dma((ny + 2, 3)),
        dma((3,)),
        dma(()),
        dma((ny,)),
    ]
    shapes = (gas_temp.shape, fuel_frac.shape, solid_temp.shape)
    held = pl.pallas_call(
        functools.partial(mega_kernel, mesh_shape),
        out_shape=tuple(pltpu.VMEM(shape, f32) for shape in shapes),
        in_specs=[ANY] * 7,
        out_specs=(VMEM,) * 3,
        scratch_shapes=scratch,
        compiler_params=pltpu.CompilerParams(vmem_limit_bytes=50 << 20, has_side_effects=True, collective_id=0),
        cost_estimate=pl.CostEstimate(flops=200_000_000, bytes_accessed=26 << 20, transcendentals=1 << 19),
        name="section",
    )(gas_temp, fuel_frac, velocity, wall_flags, solid_temp, diffusivity, gas_owner)
    return pl.pallas_call(
        store_kernel,
        out_shape=tuple(jax.ShapeDtypeStruct(shape, f32) for shape in shapes),
        in_specs=[VMEM] * 3,
        out_specs=(ANY,) * 3,
        scratch_shapes=[dma((3, PIECES))],
        compiler_params=pltpu.CompilerParams(vmem_limit_bytes=1 << 20),
        cost_estimate=pl.CostEstimate(flops=0, bytes_accessed=16 << 20, transcendentals=0),
        name="store",
    )(*held)


def solution(mesh):
    placed = (
        P("gz", "gx", "gy"),
        P("gz", "gx", "gy"),
        P(None, "gz", "gx", "gy"),
        P("gx", "gy"),
        P(None, ("gx", "gy"), "gz"),
        P(None, ("gx", "gy"), "gz"),
        P(("gx", "gy"), "gz"),
    )
    mesh_shape = tuple(mesh.shape[a] for a in ("gx", "gy", "gz"))
    return jax.shard_map(
        functools.partial(shards, mesh_shape),
        mesh=mesh,
        in_specs=placed,
        out_specs=(P("gz", "gx", "gy"), P("gz", "gx", "gy"), P(None, ("gx", "gy"), "gz")),
        check_vma=False,
    )
```
